32 devices in a mesh: rep: 4 (over y, x), fsdp: 8 (over z, core).
Axes of the slice: x: 2, y: 2, z: 4, core: 2. Of those that a mesh axis runs over, the one named last changes fastest.
Arguments:
- momentum: float32 [4, 18432, 2304], P('rep', 'fsdp'), may hold values from -60 to 60
- gradient: bfloat16 [4, 18432, 2304], P('rep', 'fsdp'), may hold values from -30 to 30
- right_factor: float32 [2304, 256], P('fsdp'), may hold values from -0.125 to 0.125
Outputs:
- new_momentum: float32 [4, 18432, 2304], P('rep', 'fsdp')
- update: bfloat16 [18432, 2304], P('fsdp')
- new_factor: float32 [2304, 256], P('fsdp')
The draws below stay inside these ranges and needn't reach their ends.
All inputs are finite; a program needn't handle non-finite values.
Results may differ from the reference program's by a relative error of at most 0.001.
Values sent between devices are 32-bit elements; how exact they have to be, the bound alone decides.
No kernel may reach another device: no remote copies, remote signals or barrier semaphores. Data moves between devices by JAX's collectives and lax.ppermute only.
A program may use at most 128 MiB of HBM per device.

```python
import math
import jax
import jax.numpy as jnp
from jax import lax

ROWS = 18432
COLS = 2304
RANK = 256
REPLICAS = 4


def column_scales(key):
    scale_key = jax.random.fold_in(key, 11)
    rising = jnp.exp(jnp.log(10.0) * jnp.arange(COLS, dtype=jnp.float32) / COLS)
    jitter = jnp.exp(jax.random.uniform(scale_key, (COLS,), jnp.float32, -0.4, 0.4))
    return 0.3 * rising * jitter


def clipped_normal(key, shape):
    return jnp.clip(jax.random.normal(key, shape, jnp.float32), -6.0, 6.0)


def draw_momentum(key, part):
    scales = column_scales(key)
    values = 2.0 * clipped_normal(jax.random.fold_in(key, 1), (REPLICAS, ROWS, COLS)) * scales
    return values.astype(jnp.float32)


def draw_gradient(key, part):
    scales = column_scales(key)
    values = clipped_normal(jax.random.fold_in(key, 2), (REPLICAS, ROWS, COLS)) * scales
    return values.astype(jnp.bfloat16)


def level_of(stream_key, shape, shards, smallest, top_value):
    gain, own = 1.0, jax.random.fold_in(stream_key, 6)
    for dim, shards_of in shards:
        draws = jnp.exp(jax.random.uniform(jax.random.fold_in(own, dim), (shards_of,), jnp.float32, smallest / len(shards), top_value / len(shards)))
        gain = gain * jnp.repeat(draws, shape[dim] // shards_of).reshape([-1 if axis == dim else 1 for axis in range(len(shape))])
    return gain


def bell_draw(stream_key, dims, width, reach, cuts=(), held_as=jnp.bfloat16):
    entries = jax.random.normal(stream_key, dims, jnp.float32) * width
    if len(cuts) > 0:
        entries = level_of(stream_key, dims, cuts, -0.22, 0.18) * entries
    return jnp.clip(entries, min=-reach, max=reach).astype(held_as)


def setup_inputs(seed: int = 0) -> dict:
    key_of = jax.random.split(jax.random.key(seed), 4)
    momentum = draw_momentum(jax.random.fold_in(key_of[3], 71), 0)
    gradient = draw_gradient(jax.random.fold_in(key_of[3], 71), 0)
    right_factor = bell_draw(key_of[2], (COLS, RANK), COLS ** -0.5, 0.125, ((0, 8),), jnp.float32)
    return {"momentum": momentum, "gradient": gradient, "right_factor": right_factor}


epsilon = 1e-06
decay_rate = 0.95
highest = lax.Precision.HIGHEST

def reference(momentum, gradient, right_factor):
    buffer = momentum + gradient.astype(jnp.float32)
    projected = jnp.einsum('irc,ck->rk', buffer, right_factor, precision=highest)
    gram_matrix = jnp.dot(projected.T.astype(jnp.float32), projected.astype(jnp.float32), precision=highest, preferred_element_type=jnp.float32)
    lower_factor = jnp.linalg.cholesky(gram_matrix)
    orthonormal = jax.scipy.linalg.solve_triangular(lower_factor, projected.T, lower=True).T
    factor = jnp.einsum('irc,rk->ck', buffer, orthonormal, precision=highest) / REPLICAS
    col_norms = jnp.sqrt(lax.optimization_barrier(jnp.sum(factor * factor, axis=0)) + epsilon)
    new_factor = factor / col_norms
    correction = jnp.dot(orthonormal.astype(jnp.float32), factor.T.astype(jnp.float32), precision=highest, preferred_element_type=jnp.float32)
    new_momentum = buffer - (1.0 - decay_rate) * correction[None]
    scaled = math.sqrt(ROWS * COLS / RANK) * jnp.dot(orthonormal.astype(jnp.float32), new_factor.T.astype(jnp.float32), precision=highest, preferred_element_type=jnp.float32)
    return (new_momentum, scaled.astype(jnp.bfloat16), new_factor)
```

```python
import functools
import math

import jax
import jax.numpy as jnp
from jax import lax
from jax.experimental import pallas as pl
from jax.experimental.pallas import tpu as pltpu
from jax.sharding import PartitionSpec as P

epsilon = 1e-06
decay_rate = 0.95
highest = lax.Precision.HIGHEST
f32, bf16 = jnp.float32, jnp.bfloat16
MiB = 1 << 20

CORE, REP, TOP = 4, 6, 10


def pick(n, unit, most):
    best = [d for d in range(unit, min(n, most) + 1, unit) if n % d == 0]
    return best[-1] if best else n


def params(mib):
    return pltpu.CompilerParams(vmem_limit_bytes=mib * MiB)


def cost(flops, nbytes):
    return pl.CostEstimate(flops=int(flops), bytes_accessed=int(nbytes), transcendentals=0)


def near(x):
    return pltpu.with_memory_space_constraint(x, pltpu.VMEM)


def split(x):
    hi = x.astype(bf16)
    return hi, (x - hi.astype(f32)).astype(bf16)


def mm(a, b, contract):
    return lax.dot_general(a, b, (contract, ((), ())), preferred_element_type=f32)


def prep_kernel(m_ref, g_ref, hi_ref, lo_ref):
    hi, lo = split(m_ref[...] + g_ref[...].astype(f32))
    hi_ref[...] = hi
    lo_ref[...] = lo


def prep(momentum, gradient):
    chunks, rows, cols = momentum.shape
    step = pick(rows, 16, 192)
    spec = pl.BlockSpec((1, step, cols), lambda c, r: (c, r, 0))
    shape = pltpu.VMEM(momentum.shape, bf16)
    return pl.pallas_call(
        prep_kernel,
        grid=(chunks, rows // step),
        in_specs=[spec, spec],
        out_specs=[spec, spec],
        out_shape=[shape, shape],
        compiler_params=params(20),
        cost_estimate=cost(10 * momentum.size * 256, 10 * momentum.size),
        name="prep",
    )(momentum, gradient)


def smem():
    return pl.BlockSpec(memory_space=pltpu.SMEM)


def vmem(n):
    return [pl.BlockSpec(memory_space=pltpu.VMEM)] * n


def right_kernel(own_at, other_at, n, idx_ref, *refs):
    hi_ref, lo_ref = refs[-2:]
    for core_at, group in ((own_at, refs[:n]), (other_at, refs[n : 2 * n])):
        for r, x_ref in enumerate(group):
            hi, lo = split(x_ref[...])
            at = idx_ref[TOP + r], slice(None), idx_ref[core_at]
            hi_ref[at] = hi
            lo_ref[at] = lo


def assemble_right(table, mine, other):
    n = len(mine)
    shape = jax.ShapeDtypeStruct((n, mine[0].shape[0], 2) + mine[0].shape[1:], bf16)
    hi, lo = pl.pallas_call(
        functools.partial(right_kernel, CORE, CORE + 1, n),
        in_specs=[smem()] + vmem(2 * n),
        out_shape=[shape, shape],
        compiler_params=params(10),
        cost_estimate=cost(1e9, 20 * mine[0].size * n),
        name="assemble_right",
    )(table, *mine, *other)
    return hi.reshape(-1, hi.shape[-1]), lo.reshape(-1, lo.shape[-1])


def add_all(refs, index=None):
    parts = [ref[...] if index is None else ref[index] for ref in refs]
    while len(parts) > 1:
        parts = [a + b for a, b in zip(parts[::2], parts[1::2])]
    return parts[0]


def pieces_kernel(n, at, idx_ref, *refs):
    for r, out_ref in enumerate(refs[n:]):
        out_ref[...] = add_all(refs[:n], idx_ref[at + r])


def add_pieces(table, at, radix, terms, count=None):
    rows, rank = terms[0].shape
    count = radix if count is None else count
    shape = jax.ShapeDtypeStruct((rows // radix, rank), f32)
    out = pl.pallas_call(
        functools.partial(pieces_kernel, len(terms), at),
        in_specs=[smem()] + vmem(len(terms)),
        out_shape=[shape] * count,
        compiler_params=params(10),
        cost_estimate=cost(1e9, 12 * rows * rank),
        name="add_pieces",
    )(table, *[t.reshape(radix, rows // radix, rank) for t in terms])
    return list(out)


def sum_kernel(*refs):
    refs[-1][...] = add_all(refs[:-1])


def add_terms(terms):
    return pl.pallas_call(
        sum_kernel,
        out_shape=jax.ShapeDtypeStruct(terms[0].shape, f32),
        compiler_params=params(10),
        cost_estimate=cost(1e9, 8 * terms[0].size),
        name="add_terms",
    )(*terms)


def order_kernel(at, idx_ref, *refs):
    for r, x_ref in enumerate(refs[:-1]):
        refs[-1][idx_ref[at + r]] = x_ref[...]


def put_in_order(table, at, parts):
    shape = (len(parts),) + parts[0].shape
    out = pl.pallas_call(
        functools.partial(order_kernel, at),
        in_specs=[smem()] + vmem(len(parts)),
        out_shape=jax.ShapeDtypeStruct(shape, f32),
        compiler_params=params(10),
        cost_estimate=cost(1e9, 8 * parts[0].size * len(parts)),
        name="put_in_order",
    )(table, *parts)
    return out.reshape(-1, shape[-1])


def project_kernel(idx_ref, hi_ref, lo_ref, vhi_ref, vlo_ref, out_ref):
    hi, lo = hi_ref[0], lo_ref[0]
    dims = ((1,), (0,))
    out_ref[...] = mm(hi, vhi_ref[...], dims) + (mm(hi, vlo_ref[...], dims) + mm(lo, vhi_ref[...], dims))


def project(table, at, hi, lo, vhi, vlo):
    _, rows, cols = hi.shape
    rank = vhi.shape[1]
    step = pick(rows, 16, 192)
    left = pl.BlockSpec((1, step, cols), lambda r, idx: (idx[at], r, 0))
    right = pl.BlockSpec((cols, rank), lambda r, idx: (0, 0))
    return pl.pallas_call(
        project_kernel,
        grid_spec=pltpu.PrefetchScalarGridSpec(
            num_scalar_prefetch=1,
            grid=(rows // step,),
            in_specs=[left, left, right, right],
            out_specs=pl.BlockSpec((step, rank), lambda r, idx: (r, 0)),
        ),
        out_shape=jax.ShapeDtypeStruct((rows, rank), f32),
        compiler_params=params(12),
        cost_estimate=cost(6 * rows * cols * rank, 4 * rows * cols),
        name="project",
    )(table, near(hi), near(lo), vhi, vlo)


def gram_kernel(a_ref, b_ref, *refs):
    gram_ref, ahi_ref, alo_ref, bhi_ref, blo_ref = refs[-5:]
    total = refs[0][...] if len(refs) == 6 else None
    for p_ref, hi_ref, lo_ref in ((a_ref, ahi_ref, alo_ref), (b_ref, bhi_ref, blo_ref)):
        p = p_ref[...]
        turned = p.T
        hi_ref[...], lo_ref[...] = split(turned)
        part = jnp.dot(turned, p, precision=highest, preferred_element_type=f32)
        total = part if total is None else total + part
    gram_ref[...] = total


def gram_call(a, b, *before):
    rows, rank = a.shape
    turned = jax.ShapeDtypeStruct((rank, rows), bf16)
    return pl.pallas_call(
        gram_kernel,
        out_shape=[jax.ShapeDtypeStruct((rank, rank), f32)] + [turned] * 4,
        compiler_params=params(16),
        cost_estimate=cost(24 * rows * rank * rank, 16 * rows * rank),
        name="gram",
    )(a, b, *before)


def factor_kernel(idx_ref, h0, h1, l0, l1, ahi, alo, bhi, blo, *rest):
    out_ref = rest[-1]
    dims = ((1,), (0,))
    big = mm(ahi[...], h0[0], dims) + mm(bhi[...], h1[0], dims)
    small = mm(ahi[...], l0[0], dims) + mm(bhi[...], l1[0], dims)
    small += mm(alo[...], h0[0], dims) + mm(blo[...], h1[0], dims)
    total = (big + small).T
    if len(rest) == 2:
        total += rest[0][...]
    out_ref[...] = total


def factor_half(idx, at, hi, lo, turned, before):
    _, rows, cols = hi.shape
    ahi = turned[0]
    rank = ahi.shape[0]
    half = cols // 2
    step = pick(half, 128, 384)
    steps = half // step
    first = pl.BlockSpec((1, rows, step), lambda c, idx: (idx[at[0]], 0, idx[at[2]] * steps + c))
    second = pl.BlockSpec((1, rows, step), lambda c, idx: (idx[at[1]], 0, idx[at[2]] * steps + c))
    whole = pl.BlockSpec((rank, rows), lambda c, idx: (0, 0))
    out = pl.BlockSpec((step, rank), lambda c, idx: (c, 0))
    extra = [] if before is None else [before]
    return pl.pallas_call(
        factor_kernel,
        grid_spec=pltpu.PrefetchScalarGridSpec(
            num_scalar_prefetch=1,
            grid=(steps,),
            in_specs=[first, second, first, second] + [whole] * 4 + [out] * len(extra),
            out_specs=out,
        ),
        out_shape=jax.ShapeDtypeStruct((half, rank), f32),
        compiler_params=params(16),
        cost_estimate=cost(12 * rows * half * rank, 8 * rows * half),
        name="factor_term",
    )(idx, near(hi), near(hi), near(lo), near(lo), *turned, *extra)


def chol_kernel(idx_ref, *refs):
    *parts, out_ref, s_ref, m_ref = refs
    n = out_ref.shape[0]
    for r, x_ref in enumerate(parts):
        rows = x_ref.shape[0]
        s_ref[pl.ds(pl.multiple_of(idx_ref[REP + r] * rows, rows), rows), :] = x_ref[...]
    b = 64 if n % 64 == 0 else n
    dot = functools.partial(jnp.dot, precision=highest, preferred_element_type=f32)
    row_id = lax.broadcasted_iota(jnp.int32, (n, n), 0)
    m_ref[...] = jnp.where(row_id == lax.broadcasted_iota(jnp.int32, (n, n), 1), 1.0, 0.0).astype(f32)
    eye = lax.broadcasted_iota(jnp.int32, (b, b), 0) == lax.broadcasted_iota(jnp.int32, (b, b), 1)
    group = 8
    local = lax.broadcasted_iota(jnp.int32, (group, 1), 0)
    for k in range(n // b):
        top, end = k * b, (k + 1) * b
        block = jnp.concatenate([s_ref[top:end, top:end], jnp.where(eye, 1.0, 0.0).astype(f32)], axis=1)
        parts = [block[i : i + group] for i in range(0, b, group)]
        for t in range(b):
            at, within = divmod(t, group)
            row = parts[at][within : within + 1]
            inverse = 1.0 / row[:, t : t + 1]
            scaled = row * inverse
            for i in range(at, b // group):
                column = parts[i][:, t : t + 1]
                if i == at:
                    column = jnp.where(local > within, column, 0.0)
                parts[i] = parts[i] - column * scaled
        block = jnp.concatenate(parts, axis=0)
        pivots = jnp.sum(jnp.where(eye, block[:, :b], 0.0), axis=1, keepdims=True)
        inverse = block[:, b:] / jnp.sqrt(pivots)
        mine = dot(inverse, m_ref[top:end, :])
        out_ref[top:end, :] = mine
        if end < n:
            upper = dot(inverse, s_ref[top:end, :])[:, end:]
            turned = upper.T
            s_ref[end:, end:] -= dot(turned, upper)
            m_ref[end:, :] -= dot(turned, mine)


def chol_inverse(table, parts):
    n = parts[0].shape[1]
    return pl.pallas_call(
        chol_kernel,
        in_specs=[smem()] + vmem(len(parts)),
        out_shape=jax.ShapeDtypeStruct((n, n), f32),
        scratch_shapes=[pltpu.VMEM((n, n), f32), pltpu.VMEM((n, n), f32)],
        compiler_params=params(6),
        cost_estimate=cost(1000 * n**3, 8 * n * n),
        name="chol_inverse",
    )(table, *parts)


def ortho_kernel(idx_ref, a_ref, b_ref, c_ref, d_ref, inv_ref, hi_ref, lo_ref):
    inv = inv_ref[...]
    for k, p_ref in enumerate((a_ref, b_ref, c_ref, d_ref)):
        q = lax.dot_general(
            p_ref[...], inv, (((1,), (1,)), ((), ())), precision=highest, preferred_element_type=f32
        )
        hi, lo = split(q)
        hi_ref[idx_ref[k]] = hi
        lo_ref[idx_ref[k]] = lo


def ortho(table, parts, inverse):
    rows, rank = parts[0].shape
    shape = jax.ShapeDtypeStruct((4, rows, rank), bf16)
    return pl.pallas_call(
        ortho_kernel,
        in_specs=[smem()] + vmem(5),
        out_shape=[shape, shape],
        compiler_params=params(16),
        cost_estimate=cost(48 * rows * rank * rank, 32 * rows * rank),
        name="ortho",
    )(table, *parts, inverse)


def norm_kernel(replicas, scale, idx_ref, mine_ref, other_ref, inv_ref, new_ref, dim_ref, hi_ref, lo_ref):
    inv = inv_ref[...]
    halves = []
    for ref in (mine_ref, other_ref):
        w = lax.dot_general(
            ref[...], inv, (((1,), (1,)), ((), ())), precision=highest, preferred_element_type=f32
        )
        halves.append(w / replicas)
    squares = [jnp.sum(f * f, axis=0, keepdims=True) for f in halves]
    norms = jnp.sqrt(squares[0] + squares[1] + epsilon)
    for c, factor in enumerate(halves):
        at = idx_ref[CORE + c]
        new = factor / norms
        new_ref[at] = new
        dim_ref[at] = ((1.0 - decay_rate) * factor).astype(bf16)
        hi_ref[at], lo_ref[at] = split(scale * new)


def normalize(table, mine, other, inverse, replicas, scale):
    rows, rank = mine.shape
    full, short = (jax.ShapeDtypeStruct((2, rows, rank), d) for d in (f32, bf16))
    out = pl.pallas_call(
        functools.partial(norm_kernel, replicas, scale),
        in_specs=[smem()] + vmem(3),
        out_shape=[full, short, short, short],
        compiler_params=params(16),
        cost_estimate=cost(24 * mine.size * rank, 28 * mine.size),
        name="normalize",
    )(table, mine, other, inverse)
    return [x.reshape(2 * rows, rank) for x in out]


def apply_kernel(hi_ref, lo_ref, qhi_ref, qlo_ref, dim_ref, fhi_ref, flo_ref, new_ref, up_ref):
    dims = ((1,), (1,))
    qhi, qlo = qhi_ref[0], qlo_ref[0]
    buffer = hi_ref[0].astype(f32) + lo_ref[0].astype(f32)
    new_ref[0] = buffer - mm(qhi, dim_ref[...], dims)
    up = mm(qhi, fhi_ref[...], dims) + (mm(qhi, flo_ref[...], dims) + mm(qlo, fhi_ref[...], dims))
    up_ref[0] = up.astype(bf16)


def apply(hi, lo, qhi, qlo, dim, fhi, flo):
    chunks, rows, cols = hi.shape
    rank = qhi.shape[2]
    step = pick(rows, 16, 192)
    wide = pl.BlockSpec((1, step, cols), lambda c, r: (c, r, 0))
    thin = pl.BlockSpec((1, step, rank), lambda c, r: (c, r, 0))
    whole = pl.BlockSpec((cols, rank), lambda c, r: (0, 0))
    return pl.pallas_call(
        apply_kernel,
        grid=(chunks, rows // step),
        in_specs=[wide, wide, thin, thin, whole, whole, whole],
        out_specs=[wide, wide],
        out_shape=[jax.ShapeDtypeStruct(hi.shape, f32), jax.ShapeDtypeStruct(hi.shape, bf16)],
        compiler_params=params(28),
        cost_estimate=cost(8 * hi.size * rank, 10 * hi.size),
        name="apply",
    )(near(hi), near(lo), qhi, qlo, dim, fhi, flo)


def digits(n):
    out, stride = [], 1
    while stride < n:
        left = n // stride
        radix = 2 if stride == 1 and left % 4 != 0 or left % 4 != 0 else 4
        if stride == 1 and n > 4:
            radix = 2
        out.append((stride, radix))
        stride *= radix
    return out


def digit(axis, stride, radix):
    return (lax.axis_index(axis) // stride) % radix


def swap(x, axis, stride, radix, r):
    pairs = []
    for i in range(lax.axis_size(axis)):
        d = (i // stride) % radix
        pairs.append((i, i + ((d ^ r) - d) * stride))
    return lax.ppermute(x, axis, pairs)


def exchange(parts, axis, stride, radix):
    return parts[:1] + [swap(parts[r], axis, stride, radix, r) for r in range(1, radix)]


def shards(momentum, gradient, right_factor):
    _, rows, cols = momentum.shape
    rank = right_factor.shape[1]
    replicas = lax.axis_size("rep")
    groups = lax.axis_size("fsdp")
    scale = math.sqrt(rows * groups * cols / rank)
    rep, own = lax.axis_index("rep"), lax.axis_index("fsdp")
    pair, *rest = digits(groups)

    low, high, core = rep & 1, rep >> 1, digit("fsdp", *pair)
    numbers = [low, 1 - low, 2 + high, 3 - high, core, 1 - core]
    numbers += [rep ^ r for r in range(replicas)]
    places = {}
    for step in reversed(rest):
        places[step] = len(numbers)
        numbers += [digit("fsdp", *step) ^ r for r in range(step[1])]
    mine = cols // groups
    table, start, momentum, gradient = lax.optimization_barrier(
        (jnp.stack(numbers).astype(jnp.int32), own * mine, momentum, gradient)
    )

    quarter = (4, rows // 4, cols)
    right = right_factor
    for step in rest[:-1]:
        right = put_in_order(table, places[step], exchange([right] * step[1], "fsdp", *step))
    top = exchange([right] * rest[-1][1], "fsdp", *rest[-1])
    hi, lo = prep(momentum.reshape(quarter), gradient.reshape(quarter))
    top[1], hi, lo = lax.optimization_barrier((top[1], hi, lo))
    top = [x.reshape(-1, mine, rank) for x in top]
    vhi, vlo = assemble_right(table, top, [swap(x, "fsdp", *pair, 1) for x in top])

    low_swap = lambda x: swap(x, "rep", 1, 2, 1)
    high_swap = lambda x: swap(x, "rep", 2, 2, 1)
    term = lambda at: project(table, at, hi, lo, vhi, vlo)
    a_send = term(1)
    b_send = term(3)
    a_came, b_came = low_swap(a_send), high_swap(b_send)
    a_keep = term(0)
    b_keep = term(2)
    a_sum, b_sum = a_keep + a_came, b_keep + b_came
    a_own, b_own = a_sum + high_swap(a_sum), b_sum + low_swap(b_sum)
    a_far, b_far = low_swap(a_own), high_swap(b_own)

    gram, *turned = gram_call(a_own, b_own)
    send = factor_half(table, (0, 2, CORE + 1), hi, lo, turned, None)
    keep = factor_half(table, (0, 2, CORE), hi, lo, turned, None)
    gram, *turned = gram_call(a_far, b_far, gram)
    send = factor_half(table, (1, 3, CORE + 1), hi, lo, turned, send)
    came = swap(send, "fsdp", *pair, 1)
    keep = factor_half(table, (1, 3, CORE), hi, lo, turned, keep)

    [part] = add_pieces(table, REP, replicas, exchange([gram] * 2, "fsdp", *pair), count=1)
    for step in rest:
        part = add_terms(exchange([part] * step[1], "fsdp", *step))
    inverse = chol_inverse(table, exchange([part] * replicas, "rep", 1, replicas))

    terms = [keep, came]
    undo = []
    for axis, step, place in [("rep", (1, replicas), REP)] + [("fsdp", d, places[d]) for d in reversed(rest)]:
        if axis == "fsdp":
            terms[0], inverse = lax.optimization_barrier((terms[0], inverse))
        if terms[0].shape[0] % step[1] == 0:
            terms = exchange(add_pieces(table, place, step[1], terms), axis, *step)
            undo.append((axis, step, place))
        else:
            terms = exchange([add_terms(terms)] * step[1], axis, *step)
    w = add_terms(terms)
    for axis, step, place in reversed(undo):
        w = put_in_order(table, place, exchange([w] * step[1], axis, *step))
    other = swap(w, "fsdp", *pair, 1)

    qhi, qlo = ortho(table, (a_own, a_far, b_own, b_far), inverse)
    new, dim, fhi, flo = normalize(table, w, other, inverse, replicas, scale)
    new_momentum, update = apply(hi, lo, qhi, qlo, dim, fhi, flo)
    new_factor = lax.dynamic_slice(new, (start, 0), (mine, rank), allow_negative_indices=False)
    return (new_momentum.reshape(momentum.shape), update.reshape(rows, cols), new_factor)


def solution(mesh):
    in_specs = (P("rep", "fsdp", None), P("rep", "fsdp", None), P("fsdp", None))
    out_specs = (P("rep", "fsdp", None), P("fsdp", None), P("fsdp", None))
    return jax.shard_map(shards, mesh=mesh, in_specs=in_specs, out_specs=out_specs, check_vma=False)
```

```python
import functools
import math

import jax
import jax.numpy as jnp
from jax import lax
from jax.experimental import pallas as pl
from jax.experimental.pallas import tpu as pltpu
from jax.sharding import PartitionSpec as P

epsilon = 1e-06
decay_rate = 0.95
highest = lax.Precision.HIGHEST
f32, bf16 = jnp.float32, jnp.bfloat16
MiB = 1 << 20

CORE, REP, HALF, TOP = 4, 6, 10, 11


def pick(n, unit, most):
    best = [d for d in range(unit, min(n, most) + 1, unit) if n % d == 0]
    return best[-1] if best else n


def params(mib):
    return pltpu.CompilerParams(vmem_limit_bytes=mib * MiB)


def cost(flops, nbytes):
    return pl.CostEstimate(flops=int(flops), bytes_accessed=int(nbytes), transcendentals=0)


def near(x):
    return pltpu.with_memory_space_constraint(x, pltpu.VMEM)


def split(x):
    hi = x.astype(bf16)
    return hi, (x - hi.astype(f32)).astype(bf16)


def mm(a, b, contract):
    return lax.dot_general(a, b, (contract, ((), ())), preferred_element_type=f32)


def prep_kernel(m_ref, g_ref, hi_ref, lo_ref):
    hi, lo = split(m_ref[...] + g_ref[...].astype(f32))
    hi_ref[...] = hi
    lo_ref[...] = lo


def prep(momentum, gradient):
    chunks, rows, cols = momentum.shape
    step = pick(rows, 16, 192)
    spec = pl.BlockSpec((1, step, cols), lambda c, r: (c, r, 0))
    shape = pltpu.VMEM(momentum.shape, bf16)
    return pl.pallas_call(
        prep_kernel,
        grid=(chunks, rows // step),
        in_specs=[spec, spec],
        out_specs=[spec, spec],
        out_shape=[shape, shape],
        compiler_params=params(8),
        cost_estimate=cost(10 * momentum.size * 256, 10 * momentum.size),
        name="prep",
    )(momentum, gradient)


def smem():
    return pl.BlockSpec(memory_space=pltpu.SMEM)


def vmem(n):
    return [pl.BlockSpec(memory_space=pltpu.VMEM)] * n


def right_kernel(own_at, other_at, n, idx_ref, *refs):
    hi_ref, lo_ref = refs[-2:]
    for core_at, group in ((own_at, refs[:n]), (other_at, refs[n : 2 * n])):
        for r, x_ref in enumerate(group):
            hi, lo = split(x_ref[...])
            at = idx_ref[TOP + r], slice(None), idx_ref[core_at]
            hi_ref[at] = hi
            lo_ref[at] = lo


def assemble_right(table, mine, other):
    n = len(mine)
    shape = jax.ShapeDtypeStruct((n, mine[0].shape[0], 2) + mine[0].shape[1:], bf16)
    hi, lo = pl.pallas_call(
        functools.partial(right_kernel, CORE, CORE + 1, n),
        in_specs=[smem()] + vmem(2 * n),
        out_shape=[shape, shape],
        compiler_params=params(6),
        cost_estimate=cost(1e9, 20 * mine[0].size * n),
        name="assemble_right",
    )(table, *mine, *other)
    return hi.reshape(-1, hi.shape[-1]), lo.reshape(-1, lo.shape[-1])


def add_all(refs, index=None):
    parts = [ref[...] if index is None else ref[index] for ref in refs]
    while len(parts) > 1:
        parts = [a + b for a, b in zip(parts[::2], parts[1::2])]
    return parts[0]


def pieces_kernel(n, at, idx_ref, *refs):
    for r, out_ref in enumerate(refs[n:]):
        out_ref[...] = add_all(refs[:n], idx_ref[at + r])


def add_pieces(table, at, radix, terms, count=None):
    rows, rank = terms[0].shape
    count = radix if count is None else count
    shape = jax.ShapeDtypeStruct((rows // radix, rank), f32)
    out = pl.pallas_call(
        functools.partial(pieces_kernel, len(terms), at),
        in_specs=[smem()] + vmem(len(terms)),
        out_shape=[shape] * count,
        compiler_params=params(5),
        cost_estimate=cost(1e9, 12 * rows * rank),
        name="add_pieces",
    )(table, *[t.reshape(radix, rows // radix, rank) for t in terms])
    return list(out)


def sum_kernel(*refs):
    refs[-1][...] = add_all(refs[:-1])


def add_terms(terms):
    return pl.pallas_call(
        sum_kernel,
        out_shape=jax.ShapeDtypeStruct(terms[0].shape, f32),
        compiler_params=params(4),
        cost_estimate=cost(1e9, 8 * terms[0].size),
        name="add_terms",
    )(*terms)


def order_kernel(at, idx_ref, *refs):
    for r, x_ref in enumerate(refs[:-1]):
        refs[-1][idx_ref[at + r]] = x_ref[...]


def put_in_order(table, at, parts):
    shape = (len(parts),) + parts[0].shape
    out = pl.pallas_call(
        functools.partial(order_kernel, at),
        in_specs=[smem()] + vmem(len(parts)),
        out_shape=jax.ShapeDtypeStruct(shape, f32),
        compiler_params=params(5),
        cost_estimate=cost(1e9, 8 * parts[0].size * len(parts)),
        name="put_in_order",
    )(table, *parts)
    return out.reshape(-1, shape[-1])


def project_kernel(idx_ref, hi_ref, lo_ref, vhi_ref, vlo_ref, out_ref):
    hi, lo = hi_ref[0], lo_ref[0]
    dims = ((1,), (0,))
    out_ref[...] = mm(hi, vhi_ref[...], dims) + (mm(hi, vlo_ref[...], dims) + mm(lo, vhi_ref[...], dims))


def project(table, at, hi, lo, vhi, vlo):
    _, rows, cols = hi.shape
    rank = vhi.shape[1]
    step = pick(rows, 16, 192)
    left = pl.BlockSpec((1, step, cols), lambda r, idx: (idx[at], r, 0))
    right = pl.BlockSpec((cols, rank), lambda r, idx: (0, 0))
    return pl.pallas_call(
        project_kernel,
        grid_spec=pltpu.PrefetchScalarGridSpec(
            num_scalar_prefetch=1,
            grid=(rows // step,),
            in_specs=[left, left, right, right],
            out_specs=pl.BlockSpec((step, rank), lambda r, idx: (r, 0)),
        ),
        out_shape=jax.ShapeDtypeStruct((rows, rank), f32),
        compiler_params=params(6),
        cost_estimate=cost(6 * rows * cols * rank, 4 * rows * cols),
        name="project",
    )(table, near(hi), near(lo), vhi, vlo)


def gram_kernel(a_ref, b_ref, *refs):
    gram_ref, ahi_ref, alo_ref, bhi_ref, blo_ref = refs[-5:]
    total = refs[0][...] if len(refs) == 6 else None
    for p_ref, hi_ref, lo_ref in ((a_ref, ahi_ref, alo_ref), (b_ref, bhi_ref, blo_ref)):
        p = p_ref[...]
        turned = p.T
        hi_ref[...], lo_ref[...] = split(turned)
        part = jnp.dot(turned, p, precision=highest, preferred_element_type=f32)
        total = part if total is None else total + part
    gram_ref[...] = total


def gram_call(a, b, *before):
    rows, rank = a.shape
    turned = jax.ShapeDtypeStruct((rank, rows), bf16)
    return pl.pallas_call(
        gram_kernel,
        out_shape=[jax.ShapeDtypeStruct((rank, rank), f32)] + [turned] * 4,
        compiler_params=params(6),
        cost_estimate=cost(24 * rows * rank * rank, 16 * rows * rank),
        name="gram",
    )(a, b, *before)


def factor_kernel(at, halves, idx_ref, h0, h1, l0, l1, ahi, alo, bhi, blo, *rest):
    *before, out_ref = rest
    width = out_ref.shape[-1]
    left = jnp.concatenate([ref[...] for ref in (ahi, alo, ahi, bhi, blo, bhi)], axis=1)
    for k in range(halves):
        cols = pl.ds(pl.multiple_of(idx_ref[at + k] * width, 128), width)
        right = jnp.concatenate([ref[0, :, cols] for ref in (h0, h0, l0, h1, h1, l1)], axis=0)
        total = mm(left, right, ((1,), (0,)))
        for ref in before:
            total += ref[k]
        out_ref[k] = total


def factor_term(table, chunks, at, halves, hi, lo, turned, *before):
    _, rows, cols = hi.shape
    rank = turned[0].shape[0]
    width = cols // 2
    first = pl.BlockSpec((1, rows, cols), lambda i, idx: (idx[chunks[0]], 0, 0))
    second = pl.BlockSpec((1, rows, cols), lambda i, idx: (idx[chunks[1]], 0, 0))
    whole = pl.BlockSpec((rank, rows), lambda i, idx: (0, 0))
    out = pl.BlockSpec((halves, rank, width), lambda i, idx: (0, 0, 0))
    extra = [pl.BlockSpec((1, rank, width), lambda i, idx, skip=skip: (skip, 0, 0)) for _, skip in before]
    return pl.pallas_call(
        functools.partial(factor_kernel, at, halves),
        grid_spec=pltpu.PrefetchScalarGridSpec(
            num_scalar_prefetch=1,
            grid=(1,),
            in_specs=[first, second, first, second] + [whole] * 4 + extra,
            out_specs=out,
        ),
        out_shape=jax.ShapeDtypeStruct((halves, rank, width), f32),
        compiler_params=params(8),
        cost_estimate=cost(12 * rows * halves * width * rank, 8 * rows * halves * width),
        name="factor_term",
    )(table, near(hi), near(hi), near(lo), near(lo), *turned, *[x for x, _ in before])


def eliminate(block):
    b = block.shape[0]
    full = (8, block.shape[1])
    spread = lambda x: jnp.broadcast_to(x, full)
    local = lax.broadcasted_iota(jnp.int32, full, 0)
    parts = [block[i : i + 8] for i in range(0, b, 8)]
    for t in range(0, b - 2, 2):
        at, within = divmod(t, 8)
        first, second = (spread(parts[at][within + i : within + i + 1]) for i in (0, 1))
        p, q, r = spread(first[:, t : t + 1]), spread(first[:, t + 1 : t + 2]), spread(second[:, t + 1 : t + 2])
        inverse = 1.0 / (p * r - q * q)
        left = (r * first - q * second) * inverse
        right = (p * second - q * first) * inverse
        for i in range(at, b // 8):
            one, two = spread(parts[i][:, t : t + 1]), spread(parts[i][:, t + 1 : t + 2])
            if i == at:
                one, two = (jnp.where(local > within + 1, x, 0.0) for x in (one, two))
            parts[i] = parts[i] - (one * left + two * right)
    block = jnp.concatenate(parts, axis=0)
    row = lax.broadcasted_iota(jnp.int32, (b, b), 0)
    col = lax.broadcasted_iota(jnp.int32, (b, b), 1)
    odd = lax.broadcasted_iota(jnp.int32, (b, 1), 0) % 2 == 1
    square, rest = block[:, :b], block[:, b:]
    pivots = jnp.sum(jnp.where(row == col, square, 0.0), axis=1, keepdims=True)
    below = jnp.sum(jnp.where(row == col + 1, square, 0.0), axis=1, keepdims=True)
    above = jnp.sum(jnp.where(row == col + 1, jnp.sum(jnp.where(row == col, square, 0.0), axis=0, keepdims=True), 0.0),
                    axis=1, keepdims=True)
    ratio = jnp.where(odd, below / jnp.where(odd, above, 1.0), 0.0)
    shifted = jnp.concatenate([rest[:1], rest[:-1]], axis=0)
    return (rest - ratio * shifted) / jnp.sqrt(pivots - ratio * below)


def chol_kernel(first, last, fresh, idx_ref, *refs):
    *parts, out_ref, s_ref, m_ref = refs
    n = out_ref.shape[0]
    b = 64 if n % 64 == 0 else n
    dot = functools.partial(jnp.dot, precision=highest, preferred_element_type=f32)
    if fresh:
        for r, x_ref in enumerate(parts):
            rows = x_ref.shape[0]
            s_ref[pl.ds(pl.multiple_of(idx_ref[REP + r] * rows, rows), rows), :] = x_ref[...]
        row, col = (lax.broadcasted_iota(jnp.int32, (n, n), d) for d in (0, 1))
        m_ref[...] = jnp.where(row == col, 1.0, 0.0).astype(f32)
    else:
        for ref, before in zip((out_ref, s_ref, m_ref), parts):
            ref[...] = before[...]
    eye = lax.broadcasted_iota(jnp.int32, (b, b), 0) == lax.broadcasted_iota(jnp.int32, (b, b), 1)
    for top in range(first, last, b):
        end = top + b
        inverse = eliminate(
            jnp.concatenate([s_ref[top:end, top:end], jnp.where(eye, 1.0, 0.0).astype(f32)], axis=1)
        )
        mine = dot(inverse, m_ref[top:end, :])
        out_ref[top:end, :] = mine
        if end < n:
            upper = dot(inverse, s_ref[top:end, :])[:, end:]
            turned = upper.T
            s_ref[end:, end:] -= dot(turned, upper)
            m_ref[end:, :] -= dot(turned, mine)


def chol_inverse(table, first, last, parts, fresh):
    n = parts[0].shape[1]
    square = jax.ShapeDtypeStruct((n, n), f32)
    return pl.pallas_call(
        functools.partial(chol_kernel, first, last, fresh),
        in_specs=[smem()] + vmem(len(parts)),
        out_shape=[square] * 3,
        compiler_params=params(4),
        cost_estimate=cost(1000 * n**3, 8 * n * n),
        name="chol_inverse",
    )(table, *parts)


def ortho_kernel(idx_ref, a_ref, b_ref, c_ref, d_ref, inv_ref, out_ref):
    inv = inv_ref[...]
    for k, p_ref in enumerate((a_ref, b_ref, c_ref, d_ref)):
        q = lax.dot_general(
            p_ref[...], inv, (((1,), (1,)), ((), ())), precision=highest, preferred_element_type=f32
        )
        hi, lo = split(q)
        out_ref[idx_ref[k]] = jnp.concatenate([hi, hi, lo], axis=1)


def ortho(table, parts, inverse):
    rows, rank = parts[0].shape
    return pl.pallas_call(
        ortho_kernel,
        in_specs=[smem()] + vmem(5),
        out_shape=jax.ShapeDtypeStruct((4, rows, 3 * rank), bf16),
        compiler_params=params(8),
        cost_estimate=cost(48 * rows * rank * rank, 40 * rows * rank),
        name="ortho",
    )(table, *parts, inverse)


def norm_kernel(replicas, scale, idx_ref, mine_ref, other_ref, inv_ref, new_ref, dim_ref, right_ref):
    inv = inv_ref[...]
    factors = [
        jnp.dot(inv, ref[...], precision=highest, preferred_element_type=f32) / replicas
        for ref in (mine_ref, other_ref)
    ]
    squares = [jnp.sum(f * f, axis=1, keepdims=True) for f in factors]
    norms = jnp.sqrt(squares[0] + squares[1] + epsilon)
    news = [f / norms for f in factors]
    for c, (factor, new) in enumerate(zip(factors, news)):
        at = idx_ref[CORE + c]
        dim_ref[at] = ((1.0 - decay_rate) * factor).astype(bf16)
        hi, lo = split(scale * new)
        right_ref[at] = jnp.concatenate([hi, lo, hi], axis=0)
    own = jnp.where(idx_ref[HALF] == idx_ref[CORE], news[0], news[1])
    new_ref[...] = own.T.reshape(new_ref.shape)


def normalize(table, mine, other, inverse, replicas, scale, shard):
    rank, width = mine.shape
    short = lambda rows: jax.ShapeDtypeStruct((2, rows, width), bf16)
    return pl.pallas_call(
        functools.partial(norm_kernel, replicas, scale),
        in_specs=[smem()] + vmem(3),
        out_shape=[jax.ShapeDtypeStruct((width, rank), f32), short(rank), short(3 * rank)],
        compiler_params=params(10),
        cost_estimate=cost(24 * mine.size * rank, 28 * mine.size),
        name="normalize",
    )(table, mine, other, inverse)


def apply_kernel(hi_ref, lo_ref, q_ref, dim_ref, right_ref, new_ref, up_ref):
    halves, rank, width = dim_ref.shape
    q = q_ref[0]
    dims = ((1,), (0,))
    for k in range(halves):
        cols = slice(k * width, (k + 1) * width)
        buffer = hi_ref[0, :, cols].astype(f32) + lo_ref[0, :, cols].astype(f32)
        new_ref[0, :, cols] = buffer - mm(q[:, :rank], dim_ref[k], dims)
        up_ref[0, :, cols] = mm(q, right_ref[k], dims).astype(bf16)


def apply(hi, lo, q, dim, right):
    chunks, rows, cols = hi.shape
    rank = dim.shape[1]
    step = pick(rows, 16, 288)
    wide = pl.BlockSpec((1, step, cols), lambda c, r: (c, r, 0))
    thin = pl.BlockSpec((1, step, 3 * rank), lambda c, r: (c, r, 0))
    whole = lambda x: pl.BlockSpec(x.shape, lambda c, r: (0, 0, 0))
    return pl.pallas_call(
        apply_kernel,
        grid=(chunks, rows // step),
        in_specs=[wide, wide, thin, whole(dim), whole(right)],
        out_specs=[wide, wide],
        out_shape=[jax.ShapeDtypeStruct(hi.shape, f32), jax.ShapeDtypeStruct(hi.shape, bf16)],
        compiler_params=params(16),
        cost_estimate=cost(8 * hi.size * rank, 10 * hi.size),
        name="apply",
    )(near(hi), near(lo), q, dim, right)


def digits(n):
    out, stride = [], 1
    while stride < n:
        left = n // stride
        radix = 2 if stride == 1 and left % 4 != 0 or left % 4 != 0 else 4
        if stride == 1 and n > 4:
            radix = 2
        out.append((stride, radix))
        stride *= radix
    return out


def digit(axis, stride, radix):
    return (lax.axis_index(axis) // stride) % radix


def swap(x, axis, stride, radix, r):
    pairs = []
    for i in range(lax.axis_size(axis)):
        d = (i // stride) % radix
        pairs.append((i, i + ((d ^ r) - d) * stride))
    return lax.ppermute(x, axis, pairs)


def exchange(parts, axis, stride, radix):
    return parts[:1] + [swap(parts[r], axis, stride, radix, r) for r in range(1, radix)]


def shards(momentum, gradient, right_factor):
    _, rows, cols = momentum.shape
    rank = right_factor.shape[1]
    replicas = lax.axis_size("rep")
    groups = lax.axis_size("fsdp")
    scale = math.sqrt(rows * groups * cols / rank)
    rep, own = lax.axis_index("rep"), lax.axis_index("fsdp")
    pair, *rest = digits(groups)

    low, high, core = rep & 1, rep >> 1, digit("fsdp", *pair)
    numbers = [low, 1 - low, 2 + high, 3 - high, core, 1 - core]
    numbers += [rep ^ r for r in range(replicas)] + [own]
    places = {}
    for step in reversed(rest):
        places[step] = len(numbers)
        numbers += [digit("fsdp", *step) ^ r for r in range(step[1])]
    mine = cols // groups
    half_groups = groups // 2
    numbers[HALF] = own // half_groups
    table, start, momentum, gradient = lax.optimization_barrier(
        (jnp.stack(numbers).astype(jnp.int32), (own % half_groups) * mine, momentum, gradient)
    )

    quarter = (4, rows // 4, cols)
    right = right_factor
    for step in rest[:-1]:
        right = put_in_order(table, places[step], exchange([right] * step[1], "fsdp", *step))
    top = exchange([right] * rest[-1][1], "fsdp", *rest[-1])
    hi, lo = prep(momentum.reshape(quarter), gradient.reshape(quarter))
    top[1], hi, lo = lax.optimization_barrier((top[1], hi, lo))
    top = [x.reshape(-1, mine, rank) for x in top]
    vhi, vlo = assemble_right(table, top, [swap(x, "fsdp", *pair, 1) for x in top])

    low_swap = lambda x: swap(x, "rep", 1, 2, 1)
    high_swap = lambda x: swap(x, "rep", 2, 2, 1)
    term = lambda at: project(table, at, hi, lo, vhi, vlo)
    a_send = term(1)
    b_send = term(3)
    a_came, b_came = low_swap(a_send), high_swap(b_send)
    a_keep = term(0)
    b_keep = term(2)
    a_sum, b_sum = a_keep + a_came, b_keep + b_came
    a_own, b_own = a_sum + high_swap(a_sum), b_sum + low_swap(b_sum)
    a_far, b_far = low_swap(a_own), high_swap(b_own)

    gram, *turned = gram_call(a_own, b_own)
    both = factor_term(table, (0, 2), CORE, 2, hi, lo, turned)
    gram, *turned = gram_call(a_far, b_far, gram)
    send = factor_term(table, (1, 3), CORE + 1, 1, hi, lo, turned, (both, 1))[0]
    came = swap(send, "fsdp", *pair, 1)
    keep = factor_term(table, (1, 3), CORE, 1, hi, lo, turned, (both, 0))[0]

    [part] = add_pieces(table, REP, replicas, exchange([gram] * 2, "fsdp", *pair), count=1)
    for step in rest:
        part = add_terms(exchange([part] * step[1], "fsdp", *step))
    blocks = exchange([part] * replicas, "rep", 1, replicas)
    block = rank // 4
    state = chol_inverse(table, 0, 2 * block, blocks, True)

    terms = exchange(add_pieces(table, REP, replicas, [keep, came]), "rep", 1, replicas)
    terms[0], *state = lax.optimization_barrier((terms[0], *state))
    undo = []
    for step in reversed(rest):
        if terms[0].shape[0] % step[1] == 0:
            terms = exchange(add_pieces(table, places[step], step[1], terms), "fsdp", *step)
            if not undo:
                state = chol_inverse(table, 2 * block, 3 * block, state, False)
                terms[1], *state = lax.optimization_barrier((terms[1], *state))
            undo.append(step)
        else:
            terms = exchange([add_terms(terms)] * step[1], "fsdp", *step)
    w = add_terms(terms)
    for step in reversed(undo):
        w = put_in_order(table, places[step], exchange([w] * step[1], "fsdp", *step))
    w, *state = lax.optimization_barrier((w, *state))
    terms = exchange([w] * replicas, "rep", 1, replicas)
    inverse = chol_inverse(table, 3 * block, rank, state, False)[0]
    q = ortho(table, (a_own, a_far, b_own, b_far), inverse)
    terms[1], inverse, q = lax.optimization_barrier((terms[1], inverse, q))
    w = put_in_order(table, REP, terms)
    other = swap(w, "fsdp", *pair, 1)

    new, dim, right = normalize(table, w, other, inverse, replicas, scale, mine)
    new_momentum, update = apply(hi, lo, q, dim, right)
    new_factor = lax.dynamic_slice(new, (start, 0), (mine, rank), allow_negative_indices=False)
    return (new_momentum.reshape(momentum.shape), update.reshape(rows, cols), new_factor)


def solution(mesh):
    in_specs = (P("rep", "fsdp", None), P("rep", "fsdp", None), P("fsdp", None))
    out_specs = (P("rep", "fsdp", None), P("fsdp", None), P("fsdp", None))
    return jax.shard_map(shards, mesh=mesh, in_specs=in_specs, out_specs=out_specs, check_vma=False)
```
